32 devices in a mesh: dp: 8 (over z, x), mp: 4 (over y, core).
Axes of the slice: x: 2, y: 2, z: 4, core: 2. Of those that a mesh axis runs over, the one named last changes fastest.
Arguments:
- teacher_states: bfloat16 [512, 128, 4096], P('dp', None, 'mp'), may hold values from -6 to 6
- teacher_gain: float32 [4096], P('mp'), may hold values from 0.25 to 1.75
- teacher_proj: bfloat16 [4096, 1024], P('mp'), may hold values from -0.09375 to 0.09375
- teacher_mask: int32 [512, 128], P('dp'), may hold values 0 or 1
- student_states: bfloat16 [1024, 64, 768], P(('dp', 'mp')), may hold values from -6 to 6
- student_gain: float32 [768], replicated, may hold values from 0.25 to 1.75
- student_proj: bfloat16 [768, 1024], replicated, may hold values from -0.21875 to 0.21875
- student_mask: int32 [1024, 64], P(('dp', 'mp')), may hold values 0 or 1
- positive: int32 [1024], P(('dp', 'mp')), may hold values from 0 to 511
Outputs:
- grad_embed: float32 [1024, 1024], P(('dp', 'mp'))
- grad_states: bfloat16 [1024, 64, 768], P(('dp', 'mp'))
The draws below stay inside these ranges and needn't reach their ends.
All inputs are finite; a program needn't handle non-finite values. No bound on the sum of `teacher_mask` or of `student_mask` on one device may be relied on, other than what follows from the above.
Results may differ from the reference program's by a relative error of at most 0.0085.
Values may be sent and summed in bfloat16 or wider, within the bound.
No kernel may reach another device: no remote copies, remote signals or barrier semaphores. Data moves between devices by JAX's collectives and lax.ppermute only.
A program may use at most 128 MiB of HBM per device.

```python
import jax
import jax.numpy as jnp
from jax import lax

D = 4096
E = 1024
DS = 768
LEN = 128
QLEN = 64
PASSAGES = 512
QUERIES = 1024


def place_ends(result, rng, least, high):
    longest = result.shape.index(max(result.shape))
    spots = []
    for shift in (0, 1):
        where = [jax.random.randint(jax.random.fold_in(rng, axis), (), 0, length) for axis, length in enumerate(result.shape)]
        where[longest] = (where[longest] + shift) % result.shape[longest]
        spots.append(tuple(where))
    return result.at[spots[0]].set(least).at[spots[1]].set(high)


def block_scale(own_key, shape, cuts, least, top_value):
    def one(dim, shards_of):
        heights = jax.random.uniform(jax.random.fold_in(jax.random.fold_in(own_key, 6), dim), (shards_of,), jnp.float32, least / len(cuts), top_value / len(cuts))
        return jnp.repeat(jnp.exp(heights), shape[dim] // shards_of).reshape((-1,) + (1,) * (len(shape) - dim - 1))

    level = one(*cuts[0])
    for cut in cuts[1:]:
        level = level * one(*cut)
    return level


def normal_values(rng, shape, spread, reach, cuts=(), kind=jnp.bfloat16):
    drawn = spread * jax.random.normal(rng, shape, jnp.float32)
    if cuts:
        drawn = drawn * block_scale(rng, shape, cuts, -0.22, 0.18)
    return jnp.clip(drawn, -reach, reach).astype(kind)


def setup_inputs(seed: int = 0) -> dict:
    streams_of = jax.random.split(jax.random.key(seed), 10)
    teacher_states = normal_values(streams_of[0], (PASSAGES, LEN, D), 1.0, 6.0, ((0, 8), (2, 4)))
    teacher_gain = jnp.clip(1.0 + 0.15 * jax.random.normal(streams_of[1], (D,), jnp.float32), 0.25, 1.75)
    teacher_proj = normal_values(streams_of[2], (D, E), D ** -0.5, 0.09375, ((0, 4),))
    teacher_mask = place_ends((jax.random.randint(streams_of[3], (PASSAGES, LEN), 0, 4) < 3).astype(jnp.int32), jax.random.fold_in(streams_of[3], 1), 0, 1)
    student_states = normal_values(streams_of[4], (QUERIES, QLEN, DS), 1.0, 6.0, ((0, 32),))
    student_gain = jnp.clip(1.0 + 0.15 * jax.random.normal(streams_of[5], (DS,), jnp.float32), 0.25, 1.75)
    student_proj = normal_values(streams_of[6], (DS, E), DS ** -0.5, 0.21875)
    student_mask = place_ends((jax.random.randint(streams_of[7], (QUERIES, QLEN), 0, 4) < 3).astype(jnp.int32), jax.random.fold_in(streams_of[7], 1), 0, 1)
    positive = place_ends(jax.random.randint(streams_of[8], (QUERIES,), 0, PASSAGES), jax.random.fold_in(streams_of[8], 1), 0, PASSAGES - 1).astype(jnp.int32)
    return dict(teacher_states=teacher_states, teacher_gain=teacher_gain, teacher_proj=teacher_proj, teacher_mask=teacher_mask, student_states=student_states, student_gain=student_gain, student_proj=student_proj, student_mask=student_mask, positive=positive)


def pool_block(pair):
    states, live_mask = pair
    values = states.astype(jnp.float32)
    scale = lax.rsqrt(lax.optimization_barrier(jnp.mean(values * values, axis=-1)) + 1e-06)
    live = live_mask.astype(jnp.float32)
    weight = live * scale
    return lax.optimization_barrier(jnp.sum(values * weight[:, :, None], axis=1))

def unit_rows(values):
    return values * lax.rsqrt(lax.optimization_barrier(jnp.mean(values * values, axis=-1, keepdims=True)) + 1e-06) / jnp.sqrt(jnp.float32(values.shape[-1]))

def student_forward(states, gain, proj, live_mask):
    values = states.astype(jnp.float32)
    scale = lax.rsqrt(lax.optimization_barrier(jnp.mean(values * values, axis=-1, keepdims=True)) + 1e-06)
    normed = (values * scale * gain).astype(jnp.bfloat16)
    flat = normed.reshape(-1, normed.shape[-1])
    act = jax.nn.gelu(jnp.dot(flat, proj, preferred_element_type=jnp.float32), approximate=True)
    act = act.reshape(states.shape[0], states.shape[1], -1)
    live = live_mask.astype(jnp.float32)
    pooled = lax.optimization_barrier(jnp.sum(act * live[:, :, None], axis=1))
    return unit_rows(pooled)

def reference(teacher_states, teacher_gain, teacher_proj, teacher_mask, student_states, student_gain, student_proj, student_mask, positive):
    blocks = teacher_states.reshape(-1, 16, LEN, D)
    masks = teacher_mask.reshape(-1, 16, LEN)
    pooled = lax.map(pool_block, (blocks, masks)).reshape(PASSAGES, D)
    tpooled = (pooled * teacher_gain).astype(jnp.bfloat16)
    traw = jnp.dot(tpooled, teacher_proj, preferred_element_type=jnp.float32)
    temb = unit_rows(traw).astype(jnp.bfloat16)
    semb, back = jax.vjp(lambda st: student_forward(st, student_gain, student_proj, student_mask), student_states)
    sround = semb.astype(jnp.bfloat16)
    tpos = temb[positive]
    tlogit = 10.0 * jnp.dot(tpos, temb.T, preferred_element_type=jnp.float32)
    slogit = 20.0 * jnp.dot(sround, temb.T, preferred_element_type=jnp.float32)
    texp = jnp.exp(tlogit)
    sexp = jnp.exp(slogit)
    diff = (sexp / lax.optimization_barrier(jnp.sum(sexp, axis=1, keepdims=True)) - texp / lax.optimization_barrier(jnp.sum(texp, axis=1, keepdims=True))).astype(jnp.bfloat16)
    grad_embed = 20.0 * jnp.dot(diff, temb, preferred_element_type=jnp.float32)
    grad_states = back(grad_embed)[0]
    return (grad_embed, grad_states.astype(jnp.bfloat16))
```

```python
import jax
import jax.numpy as jnp
from jax import lax
from jax.sharding import PartitionSpec as P

EPS = 1e-06


def unit_rows(values):
    return (
        values
        * lax.rsqrt(jnp.mean(values * values, axis=-1, keepdims=True) + EPS)
        / jnp.sqrt(jnp.float32(values.shape[-1]))
    )


def swap(values, axis, bit, size):
    return lax.ppermute(values, axis, [(i, i ^ bit) for i in range(size)])


def bits(size):
    return [1 << k for k in reversed(range(size.bit_length() - 1))]


def student_forward(states, gain, proj, live_mask):
    values = states.astype(jnp.float32)
    scale = lax.rsqrt(jnp.mean(values * values, axis=-1, keepdims=True) + EPS)
    normed = (values * scale * gain).astype(jnp.bfloat16)
    flat = normed.reshape(-1, normed.shape[-1])
    act = jax.nn.gelu(jnp.dot(flat, proj, preferred_element_type=jnp.float32), approximate=True)
    act = act.reshape(states.shape[0], states.shape[1], -1)
    live = live_mask.astype(jnp.float32)
    pooled = jnp.sum(act * live[:, :, None], axis=1)
    return unit_rows(pooled)


def shards(dp, mp, *args):
    (
        teacher_states,
        teacher_gain,
        teacher_proj,
        teacher_mask,
        student_states,
        student_gain,
        student_proj,
        student_mask,
        positive,
    ) = args
    features = teacher_states.shape[2] * mp
    rows = teacher_states.shape[0] // mp
    dp_at, mp_at = lax.axis_index("dp"), lax.axis_index("mp")

    values = teacher_states.astype(jnp.float32)
    partial_squares = jnp.sum(values * values, axis=-1)
    squares = partial_squares
    for shift in range(1, mp):
        squares = squares + swap(partial_squares, "mp", shift, mp)
    scale = lax.rsqrt(squares / features + EPS)
    weight = teacher_mask.astype(jnp.float32) * scale
    pooled = jnp.sum(values * weight[:, :, None], axis=1)
    tpooled = (pooled * teacher_gain).astype(jnp.bfloat16)
    partial = jnp.dot(tpooled, teacher_proj, preferred_element_type=jnp.float32)

    part = partial
    for bit in reversed(bits(mp)):
        high = (mp_at // bit) % 2
        groups = part.shape[0] // rows
        split = part.reshape(groups // 2, 2, rows, part.shape[-1])
        mine = lax.dynamic_index_in_dim(split, high, 1, False)
        other = lax.dynamic_index_in_dim(split, 1 - high, 1, False)
        part = (mine + swap(other, "mp", bit, mp)).reshape(-1, part.shape[-1])
    own = unit_rows(part).astype(jnp.bfloat16)

    steps = [("dp", bit, dp) for bit in bits(dp)] + [("mp", bit, mp) for bit in bits(mp)]
    last = [s for s in steps if s == ("mp", 1, mp)]
    plain = [s for s in steps if s != ("mp", 1, mp)]
    turned = list(plain)
    if ("dp", 1, dp) in plain and plain[-1] != ("dp", 1, dp):
        at = turned.index(("dp", 1, dp))
        turned[at], turned[-1] = turned[-1], turned[at]
    half = rows // 2
    sides = [own[:half][None], own[half:][None]]
    orders = [plain + last, turned + last]
    for level in range(len(steps)):
        got = [swap(sides[k], *orders[k][level]) for k in (0, 1)]
        sides = [jnp.concatenate([sides[k], got[k]]) for k in (0, 1)]
    gathered = jnp.concatenate([s.reshape(-1, own.shape[-1]) for s in sides])
    block, inside = positive // rows, positive % rows
    apart = {"dp": (block // mp) ^ dp_at, "mp": (block % mp) ^ mp_at}
    slots = []
    for order in orders:
        slot = jnp.zeros_like(positive)
        for level, (axis, bit, _) in enumerate(order):
            slot = slot + ((apart[axis] // bit) % 2) * (1 << level)
        slots.append(slot)
    place = jnp.where(
        inside < half,
        slots[0] * half + inside,
        sides[0].shape[0] * half + slots[1] * (rows - half) + inside - half,
    )

    semb, back = jax.vjp(
        lambda st: student_forward(st, student_gain, student_proj, student_mask), student_states
    )
    sround = semb.astype(jnp.bfloat16)
    columns = lax.broadcasted_iota(jnp.int32, (positive.shape[0], gathered.shape[0]), 1)
    picker = (place[:, None] == columns).astype(jnp.bfloat16)
    tpos = jnp.dot(picker, gathered, preferred_element_type=jnp.float32).astype(jnp.bfloat16)
    tlogit = 10.0 * jnp.dot(tpos, gathered.T, preferred_element_type=jnp.float32)
    slogit = 20.0 * jnp.dot(sround, gathered.T, preferred_element_type=jnp.float32)
    texp = jnp.exp(tlogit)
    sexp = jnp.exp(slogit)
    diff = (
        sexp / jnp.sum(sexp, axis=1, keepdims=True) - texp / jnp.sum(texp, axis=1, keepdims=True)
    ).astype(jnp.bfloat16)
    grad_embed = 20.0 * jnp.dot(diff, gathered, preferred_element_type=jnp.float32)
    grad_states = back(grad_embed)[0]
    return (grad_embed, grad_states)


def solution(mesh):
    in_specs = (
        P("dp", None, "mp"),
        P("mp"),
        P("mp", None),
        P("dp", None),
        P(("dp", "mp"), None, None),
        P(),
        P(),
        P(("dp", "mp"), None),
        P(("dp", "mp")),
    )
    out_specs = (P(("dp", "mp"), None), P(("dp", "mp"), None, None))
    dp, mp = mesh.shape["dp"], mesh.shape["mp"]

    def body(*args):
        return shards(dp, mp, *args)

    return jax.shard_map(body, mesh=mesh, in_specs=in_specs, out_specs=out_specs, check_vma=False)
```

```python
import functools

import jax
import jax.numpy as jnp
from jax import lax
from jax.experimental import pallas as pl
from jax.experimental.pallas import tpu as pltpu
from jax.sharding import PartitionSpec as P


EPS = 1e-06
C0 = 0.7978845608028654
C1 = C0 * 0.044715
NT = (((1,), (1,)), ((), ()))
F32, BF16 = jnp.float32, jnp.bfloat16
ROWS = 256


def column(row, length):
    spot = lax.broadcasted_iota(jnp.int32, (length, length), 0)
    lane = lax.broadcasted_iota(jnp.int32, (length, length), 1)
    return jnp.sum(jnp.where(spot == lane, row, 0.0), axis=1, keepdims=True)


def student_kernel(first, x_ref, gain_ref, proj_ref, mask_ref, slope_ref, scale_ref, raw_ref):
    queries, length = raw_ref.shape[0], mask_ref.shape[1]
    _, out = proj_ref.shape
    per = ROWS // length
    live = mask_ref[first : first + queries, :].astype(F32)
    for at in range(0, queries, per):
        top = (first + at) * length
        x = x_ref[top : top + ROWS, :].astype(F32)
        scale = lax.rsqrt(jnp.mean(x * x, axis=1, keepdims=True) + EPS)
        normed = (x * scale * gain_ref[...]).astype(BF16)
        lives = [column(live[at + q : at + q + 1, :], length) for q in range(per)]
        alive = jnp.concatenate(lives, axis=0)
        scale_ref[at * length : at * length + ROWS, :] = jnp.broadcast_to(scale * alive, (ROWS, 128))
        for col in range(0, out, 256):
            u = jnp.dot(normed, proj_ref[:, col : col + 256], preferred_element_type=F32)
            u2 = u * u
            k = C1 * u2 + C0
            t = jnp.tanh(u * k)
            half = 0.5 * t + 0.5
            act = u * half
            slope = half + (u * (0.5 - 0.5 * (t * t))) * (3.0 * C1 * u2 + C0)
            slope_ref[at * length : at * length + ROWS, col : col + 256] = slope.astype(BF16)
            for q in range(per):
                part = act[q * length : (q + 1) * length, :] * lives[q]
                raw_ref[at + q : at + q + 1, col : col + 256] = jnp.sum(part, axis=0, keepdims=True)


def student(first, queries, x, gain, proj, mask):
    length = mask.shape[1]
    vm = pl.BlockSpec(memory_space=pltpu.VMEM)
    return pl.pallas_call(
        functools.partial(student_kernel, first),
        out_shape=(
            pltpu.VMEM((queries * length, proj.shape[1]), BF16),
            pltpu.VMEM((queries * length, 128), F32),
            pltpu.VMEM((queries, proj.shape[1]), F32),
        ),
        in_specs=[vm] * 4,
        out_specs=(vm,) * 3,
        name="student",
        compiler_params=pltpu.CompilerParams(vmem_limit_bytes=12 << 20),
        cost_estimate=pl.CostEstimate(
            flops=2 * queries * length * x.shape[1] * proj.shape[1],
            bytes_accessed=queries * length * 4 * proj.shape[1],
            transcendentals=queries * length * proj.shape[1],
        ),
    )(x, gain, proj, mask)


def place_of(positive, orders, rows):
    block, inside = positive >> (rows.bit_length() - 1), positive & (rows - 1)
    apart = {"dp": (block >> 1) ^ lax.axis_index("dp"), "mp": (block ^ lax.axis_index("mp")) & 1}
    slot = jnp.zeros_like(positive)
    for k, (axis, bit, _) in enumerate(orders):
        slot = slot + jnp.where((apart[axis] & bit) != 0, 1 << k, 0)
    return slot * rows + inside


def tail_kernel(pieces, parts, orders, rows, *refs):
    positive_ref = refs[0]
    piece_refs = refs[1 : 1 + pieces]
    refs = refs[1 + pieces :]
    slope_refs, scale_refs, raw_refs = refs[:parts], refs[parts : 2 * parts], refs[2 * parts : 3 * parts]
    x_ref, gain_ref, proj_ref, embed_ref, out_ref, all_ref, buf_ref, sem = refs[3 * parts :]
    queries, wide = embed_ref.shape
    top = 0
    for piece in piece_refs:
        all_ref[top : top + piece.shape[0], :] = piece[...]
        top += piece.shape[0]
    raw = jnp.concatenate([r[...] for r in raw_refs], axis=0)
    unit = lax.rsqrt(jnp.mean(raw * raw, axis=1, keepdims=True) + EPS)
    root = 1.0 / float(wide) ** 0.5
    semb = (raw * (unit * root)).astype(BF16)
    lane = lax.broadcasted_iota(jnp.int32, (queries, top), 1)
    place = column(place_of(positive_ref[...], orders, rows).astype(F32), queries)
    picker = (lane == place.astype(jnp.int32)).astype(BF16)
    every = all_ref[...]
    tpos = jnp.dot(picker, every, preferred_element_type=F32).astype(BF16)
    both = jnp.concatenate([semb, tpos], axis=0)
    logit = lax.dot_general(both, every, NT, preferred_element_type=F32)
    sexp = jnp.exp(20.0 * logit[:queries])
    texp = jnp.exp(10.0 * logit[queries:])
    diff = sexp / jnp.sum(sexp, axis=1, keepdims=True) - texp / jnp.sum(texp, axis=1, keepdims=True)
    embed = 20.0 * jnp.dot(diff.astype(BF16), every, preferred_element_type=F32)
    embed_ref[...] = embed
    along = jnp.sum(embed * raw, axis=1, keepdims=True)
    grad = embed * (unit * root) - raw * (along * (unit * unit * unit) * (root / wide))
    grad = grad.astype(BF16)
    length = x_ref.shape[0] // queries
    width = x_ref.shape[1]
    per = ROWS // length
    copies = []
    homes = [(part, at) for part, ref in enumerate(slope_refs) for at in range(0, ref.shape[0], ROWS)]
    for block, (part, at) in enumerate(homes):
        sloped = []
        for q in range(per):
            g = grad[block * per + q : block * per + q + 1, :]
            sloped.append(slope_refs[part][at + q * length : at + (q + 1) * length, :] * g)
        sloped = jnp.concatenate(sloped, axis=0)
        down = lax.dot_general(sloped, proj_ref[...], NT, preferred_element_type=F32) * gain_ref[...]
        here = block * ROWS
        x = x_ref[here : here + ROWS, :].astype(F32)
        scale = scale_refs[part][at : at + ROWS, :][:, :1]
        pull = jnp.sum(down * x, axis=1, keepdims=True) * (scale * scale * scale) * (1.0 / width)
        buf_ref[here : here + ROWS, :] = (down * scale - x * pull).astype(BF16)
        copy = pltpu.make_async_copy(buf_ref.at[here : here + ROWS], out_ref.at[here : here + ROWS], sem.at[block])
        copy.start()
        copies.append(copy)
    for copy in copies:
        copy.wait()


def tail(positive, pieces, students, x, gain, proj, orders, rows):
    parts = len(students)
    slopes, scales, raws = zip(*students)
    queries = sum(r.shape[0] for r in raws)
    wide = proj.shape[1]
    total = sum(p.shape[0] for p in pieces)
    vm = pl.BlockSpec(memory_space=pltpu.VMEM)
    blocks = x.shape[0] // ROWS
    return pl.pallas_call(
        functools.partial(tail_kernel, len(pieces), parts, orders, rows),
        out_shape=(jax.ShapeDtypeStruct((queries, wide), F32), jax.ShapeDtypeStruct(x.shape, BF16)),
        in_specs=[vm] * (1 + len(pieces) + 3 * parts + 3),
        out_specs=(vm, pl.BlockSpec(memory_space=pl.ANY)),
        scratch_shapes=[
            pltpu.VMEM((total, wide), BF16),
            pltpu.VMEM(x.shape, BF16),
            pltpu.SemaphoreType.DMA((blocks,)),
        ],
        name="tail",
        compiler_params=pltpu.CompilerParams(vmem_limit_bytes=16 << 20),
        cost_estimate=pl.CostEstimate(
            flops=2 * x.shape[0] * x.shape[1] * wide,
            bytes_accessed=4 * x.shape[0] * x.shape[1],
            transcendentals=2 * queries * total,
        ),
    )(positive, *pieces, *slopes, *scales, *raws, x, gain, proj)


def squares_kernel(chunks, x_ref, held_ref, squares_ref, sem):
    passages, length = squares_ref.shape
    features = x_ref.shape[1]
    rows = passages * length // chunks

    def move(chunk):
        here = pl.ds(chunk * rows, rows)
        return pltpu.make_async_copy(x_ref.at[here], held_ref.at[here], sem.at[chunk])

    for chunk in range(chunks):
        move(chunk).start()
    ones = jnp.ones((8, 128), BF16)

    def step(chunk, carry):
        move(chunk).wait()
        for p in range(passages // chunks):
            top = chunk * rows + p * length
            total = None
            for col in range(0, features, 128):
                value = held_ref[pl.ds(top, length), col : col + 128].astype(F32)
                total = value * value if total is None else total + value * value
            high = total.astype(BF16)
            low = (total - high.astype(F32)).astype(BF16)
            row = lax.dot_general(ones, high, NT, preferred_element_type=F32)
            row = row + lax.dot_general(ones, low, NT, preferred_element_type=F32)
            squares_ref[pl.ds(chunk * (passages // chunks) + p, 1), :] = row[:1]
        return carry

    for chunk in range(chunks):
        step(chunk, 0)


def teacher_squares(x, passages, length):
    vm = pl.BlockSpec(memory_space=pltpu.VMEM)
    chunks = 8 if passages % 8 == 0 else 1
    x = pltpu.with_memory_space_constraint(x, pltpu.HBM)
    return pl.pallas_call(
        functools.partial(squares_kernel, chunks),
        out_shape=(pltpu.VMEM(x.shape, BF16), pltpu.VMEM((passages, length), F32)),
        in_specs=[pl.BlockSpec(memory_space=pltpu.HBM)],
        out_specs=(vm, vm),
        scratch_shapes=[pltpu.SemaphoreType.DMA((chunks,))],
        name="squares",
        compiler_params=pltpu.CompilerParams(vmem_limit_bytes=4 << 20),
        cost_estimate=pl.CostEstimate(flops=3 * x.size, bytes_accessed=2 * x.size, transcendentals=0),
    )(x)


def pool_kernel(shares, features, held_ref, mask_ref, gain_ref, proj_ref, *refs):
    square_refs, refs = refs[:shares], refs[shares:]
    outs, (weight_ref, pooled_ref, part_ref) = refs[:-3], refs[-3:]
    passages, length = mask_ref.shape
    width = held_ref.shape[1]
    total = square_refs[0][...]
    for ref in square_refs[1:]:
        total = total + ref[...]
    weight_ref[...] = mask_ref[...].astype(F32) * lax.rsqrt(total * (1.0 / features) + EPS)

    def step(group, carry):
        base = group * 8
        columns = jnp.transpose(weight_ref[pl.ds(base, 8), :])
        sums = []
        for p in range(8):
            top = (base + p) * length
            weight = jnp.broadcast_to(columns[:, p : p + 1], (length, 128))
            row = []
            for col in range(0, width, 128):
                value = held_ref[pl.ds(top, length), col : col + 128].astype(F32)
                row.append(jnp.sum(value * weight, axis=0, keepdims=True))
            sums.append(jnp.concatenate(row, axis=1))
        pooled_ref[pl.ds(base, 8), :] = jnp.concatenate(sums, axis=0)
        return carry

    for group in range(passages // 8):
        step(group, 0)
    pooled = (pooled_ref[...] * gain_ref[...]).astype(BF16)
    result = jnp.dot(pooled, proj_ref[...], preferred_element_type=F32)
    part_ref[...] = result
    rows = passages // 2
    here = lax.axis_index("mp") & 1
    for shift, out in enumerate(outs):
        top = pl.multiple_of((here ^ shift) * rows, rows)
        out[...] = part_ref[pl.ds(top, rows), :]


def teacher_pool(held, mask, gain, proj, squares, features):
    passages = mask.shape[0]
    shares, wide = len(squares), proj.shape[1]
    vm = pl.BlockSpec(memory_space=pltpu.VMEM)
    outs = [pltpu.VMEM((passages // 2, wide), F32)] * 2
    return pl.pallas_call(
        functools.partial(pool_kernel, shares, features),
        out_shape=tuple(outs),
        in_specs=[vm] * (4 + shares),
        out_specs=(vm,) * len(outs),
        scratch_shapes=[
            pltpu.VMEM(mask.shape, F32),
            pltpu.VMEM((passages, held.shape[1]), F32),
            pltpu.VMEM((passages, wide), F32),
        ],
        name="pool",
        compiler_params=pltpu.CompilerParams(vmem_limit_bytes=12 << 20),
        cost_estimate=pl.CostEstimate(flops=3 * held.size, bytes_accessed=2 * held.size, transcendentals=0),
    )(held, mask, gain, proj, *squares)


def unit_kernel(one_ref, two_ref, out_ref):
    total = one_ref[...] + two_ref[...]
    wide = total.shape[1]
    unit = lax.rsqrt(jnp.mean(total * total, axis=1, keepdims=True) + EPS)
    out_ref[...] = (total * (unit * (1.0 / float(wide) ** 0.5))).astype(BF16)


def unit_rows(one, two):
    vm = pl.BlockSpec(memory_space=pltpu.VMEM)
    return pl.pallas_call(
        unit_kernel,
        out_shape=pltpu.VMEM(one.shape, BF16),
        in_specs=[vm] * 2,
        out_specs=vm,
        name="unit",
        compiler_params=pltpu.CompilerParams(vmem_limit_bytes=4 << 20),
    )(one, two)


def swap(values, axis, bit, size):
    return lax.ppermute(values, axis, [(i, i ^ bit) for i in range(size)])


def bits(size):
    return [1 << k for k in reversed(range(size.bit_length() - 1))]


FILL = (3, 1, 2, 2)
UNIT = 4


def gather_order(dp):
    return tuple(("dp", bit, dp) for bit in bits(dp)) + (("mp", 1, 2),)


def shards(
    dp,
    mp,
    teacher_states,
    teacher_gain,
    teacher_proj,
    teacher_mask,
    student_states,
    student_gain,
    student_proj,
    student_mask,
    positive,
):
    passages, length, local = teacher_states.shape
    high = bits(mp)[:-1]

    held, square = teacher_squares(teacher_states.reshape(-1, local), passages, length)
    for bit in high:
        square = square + swap(square, "mp", bit, mp)
    squares = [square, swap(square, "mp", 1, mp)]
    tproj = pltpu.with_memory_space_constraint(teacher_proj, pltpu.VMEM)
    mine, other = teacher_pool(held, teacher_mask, teacher_gain.reshape(1, -1), tproj, squares, local * mp)

    x = student_states.reshape(-1, student_states.shape[2])
    x, proj, _ = lax.optimization_barrier((x, student_proj, square))
    xs = pltpu.with_memory_space_constraint(x, pltpu.VMEM)
    ps = pltpu.with_memory_space_constraint(proj, pltpu.VMEM)
    gain = student_gain.reshape(1, -1)
    students, first = [], 0
    for units in FILL:
        students.append(student(first, units * UNIT, xs, gain, ps, student_mask))
        first += units * UNIT
    assert first == student_mask.shape[0]

    one, two = mine, swap(other, "mp", 1, mp)
    for bit in high:
        one = one + two
        two = swap(one, "mp", bit, mp)
    side = unit_rows(one, two)
    rows = side.shape[0]
    side = side[None]
    order = gather_order(dp)
    for axis, bit, size in order[:-1]:
        side = jnp.concatenate([side, swap(side, axis, bit, size)])
    pieces = [side, swap(side, "mp", 1, mp)]
    pieces = [p.reshape(-1, p.shape[-1]) for p in pieces]
    grad_embed, grad_states = tail(positive.reshape(1, -1), pieces, students, xs, gain, ps, order, rows)
    return grad_embed, grad_states.reshape(student_states.shape)


def solution(mesh):
    in_specs = (
        P("dp", None, "mp"),
        P("mp"),
        P("mp", None),
        P("dp", None),
        P(("dp", "mp"), None, None),
        P(),
        P(),
        P(("dp", "mp"), None),
        P(("dp", "mp")),
    )
    out_specs = (P(("dp", "mp"), None), P(("dp", "mp"), None, None))
    dp, mp = mesh.shape["dp"], mesh.shape["mp"]

    def body(*args):
        return shards(dp, mp, *args)

    return jax.shard_map(body, mesh=mesh, in_specs=in_specs, out_specs=out_specs, check_vma=False)
```
